256 devices in a mesh: job: 2 (over y), fsdp: 64 (over x, z), tp: 2 (over core).
Axes of the slice: x: 4, y: 2, z: 16, core: 2. Of those that a mesh axis runs over, the one named last changes fastest.
The devices are a block of a 4x16x16 slice.
Arguments:
- weight: bfloat16 [8192, 16384], P(('job', 'fsdp'), 'tp'), parts along dimension 0, may hold values from -0.09375 to 0.09375
- grad: bfloat16 [8192, 16384], P(('job', 'fsdp'), 'tp'), parts along dimension 0, may hold values from -36 to 36
- row_moment: float32 [8192], P(('job', 'fsdp')), parts along dimension 0, may hold values from 0.01 to 10
- col_moment: float32 [32768], P(('job', 'tp')), parts along dimension 0, may hold values from 0.01 to 10
- states: bfloat16 [6144, 4096], P(('job', 'fsdp')), parts along dimension 0, may hold values from -6 to 6
- norm_gain: bfloat16 [8192], P('job'), parts along dimension 0, may hold values from 0.099609375 to 1.8984375
- gate_values: bfloat16 [6144, 16384], P(('job', 'fsdp'), 'tp'), parts along dimension 0, may hold values from -8 to 8
Outputs:
- new_weight: bfloat16 [8192, 16384], P(('job', 'fsdp'), 'tp'), parts along dimension 0
- new_rows: float32 [8192], P(('job', 'fsdp')), parts along dimension 0
- new_columns: float32 [32768], P(('job', 'tp')), parts along dimension 0
- hidden: bfloat16 [6144, 16384], P(('job', 'fsdp'), 'tp'), parts along dimension 0
The draws below stay inside these ranges and needn't reach their ends.
There are 2 independent parts, one for each index of `job`. The reference program is written for one: setup_inputs(seed, part) draws one part's arguments, and reference() takes and returns one part's arrays. A program takes and returns all parts, laid end to end along the dimension named above; each array names one. Nothing has to cross between parts.
All inputs are finite; a program needn't handle non-finite values.
Results may differ from the reference program's by a relative error of at most 0.002.
The reference program's roundings to bfloat16 on the way (of `normed` and `up_values`) count: a program that leaves them out, or rounds other values in their place, can miss the bound.
Values may be sent and summed in bfloat16 or wider, within the bound.
No kernel may reach another device: no remote copies, remote signals or barrier semaphores. Data moves between devices by JAX's collectives and lax.ppermute only.
A program may use at most 128 MiB of HBM per device.

```python
import math
import jax
import jax.numpy as jnp
from jax import lax

D = 4096
FF = 16384
TOKENS = 3072


def draw_grad(key, part):
    row_key, col_key, random_key = jax.random.split(key, 3)
    row_place = jnp.arange(D).astype(jnp.float32) / (D - 1)
    col_place = jnp.arange(FF).astype(jnp.float32) / (FF - 1)
    row_draw = jax.random.uniform(row_key, (D,), jnp.float32)
    col_draw = jax.random.uniform(col_key, (FF,), jnp.float32)
    row_scale = 0.1 * jnp.exp(math.log(10.0) * row_draw + math.log(3.0) * row_place)
    col_scale = 0.1 * jnp.exp(math.log(10.0) * col_draw + math.log(3.0) * col_place)
    random_part = jax.random.truncated_normal(random_key, -4.0, 4.0, (D, FF), jnp.float32)
    return (random_part * row_scale[:, None] * col_scale[None, :]).astype(jnp.bfloat16)


def block_scale(stream_key, shape, pieces, smallest, top_value):
    gain, own = 1.0, jax.random.fold_in(stream_key, 6)
    for position, shards_of in pieces:
        heights = jnp.exp(jax.random.uniform(jax.random.fold_in(own, position), (shards_of,), jnp.float32, smallest / len(pieces), top_value / len(pieces)))
        gain = gain * jnp.repeat(heights, shape[position] // shards_of).reshape([-1 if axis == position else 1 for axis in range(len(shape))])
    return gain


def normal_values(rng, extent, deviation, bound, pieces=(), dtype=jnp.bfloat16):
    loudness = block_scale(rng, extent, pieces, -0.22, 0.18) if pieces else 1.0
    drawn = jax.random.normal(rng, extent, jnp.float32) * deviation * loudness
    return jnp.minimum(jnp.maximum(drawn, -bound), bound).astype(dtype)


def setup_inputs(seed: int = 0, part: int = 0) -> dict:
    seeds = jax.random.split(jax.random.key(seed), 8)
    own_keys = jax.random.split(jax.random.fold_in(seeds[7], part), 8)
    weight = normal_values(own_keys[0], (D, FF), D ** -0.5, 0.09375, ((0, 64), (1, 2)))
    grad = draw_grad(jax.random.fold_in(jax.random.fold_in(seeds[7], part), 71), part)
    row_moment = jnp.clip(jnp.exp(math.log(10.0) - 6.9077553 * jax.random.uniform(own_keys[2], (D,), jnp.float32) ** block_scale(own_keys[2], (D,), ((0, 64),), -0.2, 0.2)), 0.01, 10.0)
    col_moment = jnp.clip(jnp.exp(math.log(10.0) - 6.9077553 * jax.random.uniform(own_keys[3], (FF,), jnp.float32) ** block_scale(own_keys[3], (FF,), ((0, 2),), -0.2, 0.2)), 0.01, 10.0)
    states = normal_values(own_keys[4], (TOKENS, D), 1.0, 6.0, ((0, 64),))
    norm_gain = jnp.clip(1.0 + 0.18 * jax.random.normal(own_keys[5], (D,), jnp.float32), 0.099609375, 1.8984375).astype(jnp.bfloat16)
    gate_values = normal_values(own_keys[6], (TOKENS, FF), 2.0, 8.0, ((0, 64), (1, 2)))
    return {"weight": weight, "grad": grad, "row_moment": row_moment, "col_moment": col_moment, "states": states, "norm_gain": norm_gain, "gate_values": gate_values}


def reference(weight, grad, row_moment, col_moment, states, norm_gain, gate_values):
    gradient = grad.astype(jnp.float32)
    squares = gradient * gradient + 1e-30
    row_mean = lax.optimization_barrier(jnp.mean(squares, axis=1))
    col_mean = lax.optimization_barrier(jnp.mean(squares, axis=0))
    new_rows = 0.8 * row_moment + 0.2 * row_mean
    new_columns = 0.8 * col_moment + 0.2 * col_mean
    row_scale = jnp.mean(new_rows)
    update = gradient / jnp.sqrt(new_rows[:, None] * new_columns[None, :] / row_scale)
    new_weight = (weight.astype(jnp.float32) - 0.01 * update).astype(jnp.bfloat16)
    values = states.astype(jnp.float32)
    normed = (values * lax.rsqrt(lax.optimization_barrier(jnp.mean(values * values, axis=1, keepdims=True)) + 1e-06) * norm_gain.astype(jnp.float32)).astype(jnp.bfloat16)
    up_values = jnp.dot(normed, new_weight, preferred_element_type=jnp.float32).astype(jnp.bfloat16)
    hidden = (jax.nn.silu(gate_values.astype(jnp.float32)) * up_values.astype(jnp.float32)).astype(jnp.bfloat16)
    return (new_weight, new_rows, new_columns, hidden)
```

```python
import jax
import jax.numpy as jnp
from jax import lax
from jax.sharding import Mesh
from jax.sharding import PartitionSpec as P

JOB_FSDP = ("job", "fsdp_0", "fsdp_1")
X, Z = "fsdp_0", "fsdp_1"
CHUNKS = 2


def from_each(x, axis):
    size, me = lax.axis_size(axis), lax.axis_index(axis)
    yield me, x
    for step in sorted(range(1, size), key=lambda k: min(k, size - k)):
        moved = lax.ppermute(x, axis, [(i, (i + step) % size) for i in range(size)])
        yield lax.rem(me - step + size, size), moved


def scatter_sum(x, axis):
    size, me = lax.axis_size(axis), lax.axis_index(axis)
    blocks = x.reshape(size, -1)
    total = lax.dynamic_index_in_dim(blocks, me, 0, keepdims=False)
    for step in sorted(range(1, size), key=lambda k: min(k, size - k)):
        block = lax.dynamic_index_in_dim(blocks, lax.rem(me + step, size), 0, keepdims=False)
        total += lax.ppermute(block, axis, [(i, (i + step) % size) for i in range(size)])
    return total


def gather(x, axis):
    out = jnp.zeros((lax.axis_size(axis), *x.shape), x.dtype)
    for source, moved in from_each(x, axis):
        out = lax.dynamic_update_index_in_dim(out, moved, source, 0)
    return out


def on_device(weight, grad, row_moment, col_moment, states, norm_gain, gate_values):
    n_x, n_z, n_tp = lax.axis_size(X), lax.axis_size(Z), lax.axis_size("tp")
    local_rows, local_columns = grad.shape
    columns = local_columns * n_tp
    rows = local_rows * n_x * n_z
    values = states.astype(jnp.float32)
    normed = (
        values
        * lax.rsqrt(jnp.mean(values * values, axis=1, keepdims=True) + 1e-06)
        * norm_gain.astype(jnp.float32)
    ).astype(jnp.bfloat16)
    tokens = lax.all_gather(normed, Z, axis=0, tiled=True)

    gradient = grad.astype(jnp.float32)
    squares = gradient * gradient + 1e-30
    row_partial = jnp.sum(squares, axis=1)
    col_partial = jnp.sum(squares, axis=0)
    row_total = row_partial + lax.ppermute(row_partial, "tp", [(0, 1), (1, 0)])
    new_rows = 0.8 * row_moment + 0.2 * (row_total / columns)
    mine = jnp.concatenate([scatter_sum(col_partial, X), jnp.full((128,), jnp.sum(new_rows) / 128)])
    mine = lax.all_to_all(jnp.broadcast_to(mine, (n_z, *mine.shape)), Z, 0, 0).sum(axis=0)
    quarters = gather(mine, X)
    col_total = quarters[:, :-128].reshape(-1)
    rows_summed = jnp.sum(quarters[:, -128:])
    new_columns = 0.8 * col_moment + 0.2 * (col_total / rows)
    row_scale = rows_summed / rows
    update = gradient / jnp.sqrt(new_rows[:, None] * new_columns[None, :] / row_scale)
    new_weight = (weight.astype(jnp.float32) - 0.01 * update).astype(jnp.bfloat16)

    width = local_columns // CHUNKS
    hidden = []
    for c in range(CHUNKS):
        part = slice(c * width, (c + 1) * width)
        block = lax.all_to_all(new_weight[:, part], Z, split_axis=1, concat_axis=0, tiled=True)
        block = gather(block, X).reshape(rows, -1)
        up = jnp.dot(tokens, block, preferred_element_type=jnp.float32).astype(jnp.bfloat16)
        up = lax.all_to_all(up, Z, split_axis=0, concat_axis=1, tiled=True)
        gate = jax.nn.silu(gate_values[:, part].astype(jnp.float32))
        hidden.append((gate * up.astype(jnp.float32)).astype(jnp.bfloat16))
    return (new_weight, new_rows, new_columns, jnp.concatenate(hidden, axis=1))


def solution(mesh):
    job, fsdp, tp = (mesh.shape[n] for n in ("job", "fsdp", "tp"))
    finer = Mesh(mesh.devices.reshape(job, 4, fsdp // 4, tp), ("job", X, Z, "tp"))
    placed = (
        P(JOB_FSDP, "tp"),
        P(JOB_FSDP, "tp"),
        P(JOB_FSDP),
        P(("job", "tp")),
        P(JOB_FSDP, None),
        P("job"),
        P(JOB_FSDP, "tp"),
    )
    return jax.shard_map(
        on_device,
        mesh=finer,
        in_specs=placed,
        out_specs=(P(JOB_FSDP, "tp"), P(JOB_FSDP), P(("job", "tp")), P(JOB_FSDP, "tp")),
        check_vma=False,
    )
```

```python
import jax
import jax.numpy as jnp
from jax import lax
from jax.sharding import Mesh
from jax.sharding import PartitionSpec as P

JOB_FSDP = ("job", "fsdp_0", "fsdp_1")
X, Z = "fsdp_0", "fsdp_1"
CHUNKS = 2


def from_each(x, axis):
    size, me = lax.axis_size(axis), lax.axis_index(axis)
    yield me, x
    for step in sorted(range(1, size), key=lambda k: min(k, size - k)):
        moved = lax.ppermute(x, axis, [(i, (i + step) % size) for i in range(size)])
        yield lax.rem(me - step + size, size), moved


def scatter_sum(x, axis):
    size, me = lax.axis_size(axis), lax.axis_index(axis)
    blocks = x.reshape(size, -1)
    total = lax.dynamic_index_in_dim(blocks, me, 0, keepdims=False)
    for step in sorted(range(1, size), key=lambda k: min(k, size - k)):
        block = lax.dynamic_index_in_dim(blocks, lax.rem(me + step, size), 0, keepdims=False)
        total += lax.ppermute(block, axis, [(i, (i + step) % size) for i in range(size)])
    return total


def gather(x, axis):
    out = jnp.zeros((lax.axis_size(axis), *x.shape), x.dtype)
    for source, moved in from_each(x, axis):
        out = lax.dynamic_update_index_in_dim(out, moved, source, 0)
    return out


def dot(a, b):
    return jnp.dot(a, b, preferred_element_type=jnp.float32)


def step(weight, grad, row_moment, col_moment, states, norm_gain, gate_values):
    n_x, n_z, n_tp = lax.axis_size(X), lax.axis_size(Z), lax.axis_size("tp")
    local_rows, local_columns = grad.shape
    columns = local_columns * n_tp
    rows = local_rows * n_x * n_z
    gradient = grad.astype(jnp.float32)
    squares = gradient * gradient + 1e-30
    row_partial = jnp.sum(squares, axis=1)
    col_partial = jnp.sum(squares, axis=0)
    states, col_partial = lax.optimization_barrier((states, col_partial))
    values = states.astype(jnp.float32)
    scale = lax.rsqrt(jnp.mean(values * values, axis=1, keepdims=True) + 1e-06)
    share = states.shape[1] // n_tp
    my_share = lax.axis_index("tp") * share
    normed = (
        lax.dynamic_slice_in_dim(states, my_share, share, 1).astype(jnp.float32)
        * scale
        * lax.dynamic_slice_in_dim(norm_gain, my_share, share, 0).astype(jnp.float32)
    ).astype(jnp.bfloat16)
    tokens = lax.all_gather(normed, Z, axis=0, tiled=True)
    other_tokens = lax.ppermute(tokens, "tp", [(0, 1), (1, 0)])
    row_total = row_partial + lax.ppermute(row_partial, "tp", [(0, 1), (1, 0)])
    new_rows = 0.8 * row_moment + 0.2 * (row_total / columns)
    mine = jnp.concatenate([scatter_sum(col_partial, X), jnp.full((128,), jnp.sum(new_rows) / 128)])
    mine = lax.all_to_all(jnp.broadcast_to(mine, (n_z, *mine.shape)), Z, 0, 0).sum(axis=0)
    quarters = gather(mine, X)
    col_total = quarters[:, :-128].reshape(-1)
    rows_summed = jnp.sum(quarters[:, -128:])
    new_columns = 0.8 * col_moment + 0.2 * (col_total / rows)
    row_scale = rows_summed / rows
    update = gradient / jnp.sqrt(new_rows[:, None] * new_columns[None, :] / row_scale)
    new_weight = (weight.astype(jnp.float32) - 0.01 * update).astype(jnp.bfloat16)

    width = local_columns // CHUNKS
    hidden, ups = [], []
    for c in range(CHUNKS):
        part = slice(c * width, (c + 1) * width)
        block = lax.all_to_all(new_weight[:, part], Z, split_axis=1, concat_axis=0, tiled=True)
        if ups:
            block, ups[-1] = lax.optimization_barrier((block, ups[-1]))
        block = gather(block, X).reshape(rows, -1)
        up = dot(tokens, lax.dynamic_slice_in_dim(block, my_share, share, 0))
        up += dot(other_tokens, lax.dynamic_slice_in_dim(block, share - my_share, share, 0))
        ups.append(up.astype(jnp.bfloat16))
    for c, up in enumerate(ups):
        part = slice(c * width, (c + 1) * width)
        up = lax.all_to_all(up, Z, split_axis=0, concat_axis=1, tiled=True)
        gate = jax.nn.silu(gate_values[:, part].astype(jnp.float32))
        hidden.append((gate * up.astype(jnp.float32)).astype(jnp.bfloat16))
    return (new_weight, new_rows, new_columns, jnp.concatenate(hidden, axis=1))


def solution(mesh):
    job, fsdp, tp = (mesh.shape[n] for n in ("job", "fsdp", "tp"))
    finer = Mesh(mesh.devices.reshape(job, 4, fsdp // 4, tp), ("job", X, Z, "tp"))
    placed = (
        P(JOB_FSDP, "tp"),
        P(JOB_FSDP, "tp"),
        P(JOB_FSDP),
        P(("job", "tp")),
        P(JOB_FSDP, None),
        P("job"),
        P(JOB_FSDP, "tp"),
    )
    return jax.shard_map(
        step,
        mesh=finer,
        in_specs=placed,
        out_specs=(P(JOB_FSDP, "tp"), P(JOB_FSDP), P(("job", "tp")), P(JOB_FSDP, "tp")),
        check_vma=False,
    )
```

```python
import jax
import jax.numpy as jnp
from jax import lax
from jax.sharding import Mesh
from jax.sharding import PartitionSpec as P

JOB_FSDP = ("job", "fsdp_0", "fsdp_1")
X, Z = "fsdp_0", "fsdp_1"
CHUNKS = 2


def from_each(x, axis):
    size, me = lax.axis_size(axis), lax.axis_index(axis)
    yield me, x
    for step in sorted(range(1, size), key=lambda k: min(k, size - k)):
        moved = lax.ppermute(x, axis, [(i, (i + step) % size) for i in range(size)])
        yield lax.rem(me - step + size, size), moved


def scatter_sum(x, axis):
    size, me = lax.axis_size(axis), lax.axis_index(axis)
    blocks = x.reshape(size, -1)
    total = lax.dynamic_index_in_dim(blocks, me, 0, keepdims=False)
    for step in sorted(range(1, size), key=lambda k: min(k, size - k)):
        block = lax.dynamic_index_in_dim(blocks, lax.rem(me + step, size), 0, keepdims=False)
        total += lax.ppermute(block, axis, [(i, (i + step) % size) for i in range(size)])
    return total


def gather(x, axis):
    out = jnp.zeros((lax.axis_size(axis), *x.shape), x.dtype)
    for source, moved in from_each(x, axis):
        out = lax.dynamic_update_index_in_dim(out, moved, source, 0)
    return out


def ring_gather(x, axis):
    size, me = lax.axis_size(axis), lax.axis_index(axis)
    x = lax.optimization_barrier(x)
    out = jnp.zeros((size, *x.shape), x.dtype)
    out = lax.dynamic_update_index_in_dim(out, x, me, 0)
    right = left = x
    for step in range(1, size // 2 + 1):
        right = lax.ppermute(right, axis, [(i, (i + 1) % size) for i in range(size)])
        if step < size - step:
            left = lax.ppermute(left, axis, [((i + 1) % size, i) for i in range(size)])
        out = lax.dynamic_update_index_in_dim(out, right, lax.rem(me - step + size, size), 0)
        if step < size - step:
            out = lax.dynamic_update_index_in_dim(out, left, lax.rem(me + step, size), 0)
    return out


def dot(a, b):
    return jnp.dot(a, b, preferred_element_type=jnp.float32)


def step(weight, grad, row_moment, col_moment, states, norm_gain, gate_values):
    n_x, n_z, n_tp = lax.axis_size(X), lax.axis_size(Z), lax.axis_size("tp")
    local_rows, local_columns = grad.shape
    columns = local_columns * n_tp
    rows = local_rows * n_x * n_z
    share = states.shape[1] // n_tp
    my_share = lax.axis_index("tp") * share
    tokens = ring_gather(lax.dynamic_slice_in_dim(states, my_share, share, 1), Z)
    other_tokens = lax.ppermute(tokens, "tp", [(0, 1), (1, 0)])
    gradient = grad.astype(jnp.float32)
    squares = gradient * gradient + 1e-30
    row_partial = jnp.sum(squares, axis=1)
    col_partial = jnp.sum(squares, axis=0)
    values = states.astype(jnp.float32)
    scale = lax.rsqrt(jnp.mean(values * values, axis=1) + 1e-06)
    row_total = row_partial + lax.ppermute(row_partial, "tp", [(0, 1), (1, 0)])
    new_rows = 0.8 * row_moment + 0.2 * (row_total / columns)
    quarter = scatter_sum(col_partial, X)
    n_quarter = quarter.shape[0]
    extra = jnp.zeros((128,), jnp.float32).at[: scale.shape[0]].set(scale)
    extra = extra.at[-1].set(jnp.sum(new_rows))
    mine = jnp.concatenate([quarter, extra])
    theirs = lax.all_to_all(jnp.broadcast_to(mine, (n_z, *mine.shape)), Z, 0, 0)
    scales = theirs[:, n_quarter : n_quarter + scale.shape[0]].reshape(-1, 1)
    mine = theirs.sum(axis=0)
    quarters = gather(mine, X)
    col_total = quarters[:, :-128].reshape(-1)
    rows_summed = jnp.sum(quarters[:, -1])
    new_columns = 0.8 * col_moment + 0.2 * (col_total / rows)
    row_scale = rows_summed / rows
    update = gradient / jnp.sqrt(new_rows[:, None] * new_columns[None, :] / row_scale)
    new_weight = (weight.astype(jnp.float32) - 0.01 * update).astype(jnp.bfloat16)

    def normed(part, start):
        gain = lax.dynamic_slice_in_dim(norm_gain, start, share, 0).astype(jnp.float32)
        return (part.reshape(-1, share).astype(jnp.float32) * scales * gain).astype(jnp.bfloat16)

    tokens = normed(tokens, my_share)
    other_tokens = normed(other_tokens, share - my_share)
    width = local_columns // CHUNKS
    hidden, ups = [], []
    for c in range(CHUNKS):
        part = slice(c * width, (c + 1) * width)
        block = lax.all_to_all(new_weight[:, part], Z, split_axis=1, concat_axis=0, tiled=True)
        if ups:
            block, ups[-1] = lax.optimization_barrier((block, ups[-1]))
        block = gather(block, X).reshape(rows, -1)
        up = dot(tokens, lax.dynamic_slice_in_dim(block, my_share, share, 0))
        up += dot(other_tokens, lax.dynamic_slice_in_dim(block, share - my_share, share, 0))
        ups.append(up.astype(jnp.bfloat16))
    for c, up in enumerate(ups):
        part = slice(c * width, (c + 1) * width)
        up = lax.all_to_all(up, Z, split_axis=0, concat_axis=1, tiled=True)
        gate = jax.nn.silu(gate_values[:, part].astype(jnp.float32))
        hidden.append((gate * up.astype(jnp.float32)).astype(jnp.bfloat16))
    return (new_weight, new_rows, new_columns, jnp.concatenate(hidden, axis=1))


def solution(mesh):
    job, fsdp, tp = (mesh.shape[n] for n in ("job", "fsdp", "tp"))
    finer = Mesh(mesh.devices.reshape(job, 4, fsdp // 4, tp), ("job", X, Z, "tp"))
    placed = (
        P(JOB_FSDP, "tp"),
        P(JOB_FSDP, "tp"),
        P(JOB_FSDP),
        P(("job", "tp")),
        P(JOB_FSDP, None),
        P("job"),
        P(JOB_FSDP, "tp"),
    )
    return jax.shard_map(
        step,
        mesh=finer,
        in_specs=placed,
        out_specs=(P(JOB_FSDP, "tp"), P(JOB_FSDP), P(("job", "tp")), P(JOB_FSDP, "tp")),
        check_vma=False,
    )
```

```python
import jax
import jax.numpy as jnp
from jax import lax
from jax.experimental import pallas as pl
from jax.experimental.pallas import tpu as pltpu
from jax.sharding import Mesh
from jax.sharding import PartitionSpec as P

JOB_FSDP = ("job", "fsdp_0", "fsdp_1")
X, Z = "fsdp_0", "fsdp_1"
CHUNKS = 2
LANES = 128
VMEM_LIMIT = 16 * 2**20


def steps(size):
    return sorted(range(size), key=lambda k: min(k, size - k))


def shifted(x, axis, step):
    size = lax.axis_size(axis)
    return x if step == 0 else lax.ppermute(x, axis, [(i, (i + step) % size) for i in range(size)])


def scatter_sum(x, axis):
    size, me = lax.axis_size(axis), lax.axis_index(axis)
    blocks = x.reshape(size, -1, x.shape[1])
    total = 0
    for step in steps(size):
        block = lax.dynamic_index_in_dim(blocks, lax.rem(me + step, size), 0, keepdims=False)
        total += shifted(block, axis, step)
    return total


def dot(a, b):
    return jnp.dot(a, b, preferred_element_type=jnp.float32)


def vmem(n):
    return [pl.BlockSpec(memory_space=pltpu.VMEM)] * n


def apply_update(pieces, me, col_moment, new_rows, grad, weight, n_z, rows):
    size, local_rows, local_columns = len(pieces), *grad.shape
    share = col_moment.shape[0] // size
    width = local_columns // CHUNKS // n_z

    def kernel(me_ref, *refs):
        piece_refs, refs = refs[:size], refs[size:]
        moment_ref, rows_ref, grad_ref, weight_ref, out_ref, columns_ref, *send_refs, factor_ref = refs
        rows_summed = 0.0
        for step, piece_ref in zip(steps(size), piece_refs, strict=True):
            source = lax.rem(me_ref[0] - step + size, size)
            place = pl.ds(pl.multiple_of(source * share, share), share)
            factor_ref[place, :] = piece_ref[:share, :]
            rows_summed += piece_ref[share : share + 1, LANES - 1 :]
        new_columns = 0.8 * moment_ref[...] + 0.2 * (factor_ref[...] / rows)
        columns_ref[...] = new_columns
        factor_ref[...] = 0.01 * jnp.sqrt((rows_summed / rows) / new_columns)
        row_factor = jnp.broadcast_to(1.0 / jnp.sqrt(rows_ref[...]), (local_rows, LANES))
        for group in range(local_columns // LANES):
            at = group * LANES
            part = slice(at, at + LANES)
            scaled = grad_ref[:, part].astype(jnp.float32) * row_factor * factor_ref[group : group + 1, :]
            new = (weight_ref[:, part].astype(jnp.float32) - scaled).astype(jnp.bfloat16)
            out_ref[:, part] = new
            chunk, rest = divmod(at, width * n_z)
            target, rest = divmod(rest, width)
            send_refs[chunk][target, :, rest : rest + LANES] = new

    send = jax.ShapeDtypeStruct((n_z, local_rows, width), jnp.bfloat16)
    return pl.pallas_call(
        kernel,
        out_shape=[
            jax.ShapeDtypeStruct(grad.shape, jnp.bfloat16),
            jax.ShapeDtypeStruct(col_moment.shape, jnp.float32),
            *[send] * CHUNKS,
        ],
        in_specs=[pl.BlockSpec(memory_space=pltpu.SMEM), *vmem(size + 4)],
        out_specs=vmem(2 + CHUNKS),
        scratch_shapes=[pltpu.VMEM(col_moment.shape, jnp.float32)],
        compiler_params=pltpu.CompilerParams(vmem_limit_bytes=VMEM_LIMIT),
    )(me.reshape(1), *pieces, col_moment, new_rows.reshape(-1, 1), grad, weight)


def finish(up, gate, hidden, chunk):
    n_z, tokens, width = up.shape

    def kernel(up_ref, gate_ref, *refs):
        out_ref = refs[-1]
        for z in range(n_z):
            part = slice(z * width, (z + 1) * width)
            v = gate_ref[:, part].astype(jnp.float32)
            out_ref[:, part] = (v / (1.0 + jnp.exp(-v)) * up_ref[z].astype(jnp.float32)).astype(jnp.bfloat16)

    block = pl.BlockSpec((tokens, n_z * width), lambda i: (0, chunk))
    first = hidden is None
    return pl.pallas_call(
        kernel,
        grid=(1,),
        out_shape=jax.ShapeDtypeStruct(gate.shape, jnp.bfloat16),
        in_specs=[pl.BlockSpec(up.shape, lambda i: (0, 0, 0)), block]
        + ([] if first else [pl.BlockSpec(memory_space=pl.ANY)]),
        out_specs=block,
        input_output_aliases={} if first else {2: 0},
        compiler_params=pltpu.CompilerParams(vmem_limit_bytes=VMEM_LIMIT),
    )(up, gate, *([] if first else [hidden]))


def step(weight, grad, row_moment, col_moment, states, norm_gain, gate_values):
    n_x, n_z, n_tp = lax.axis_size(X), lax.axis_size(Z), lax.axis_size("tp")
    me_x, me_tp = lax.axis_index(X), lax.axis_index("tp")
    local_rows, local_columns = grad.shape
    columns = local_columns * n_tp
    rows = local_rows * n_x * n_z
    values = states.astype(jnp.float32)
    scale = lax.rsqrt(jnp.mean(values * values, axis=1) + 1e-06)

    features = states.shape[1]
    share, piece = features // n_tp, features // n_x
    tokens = lax.dynamic_slice_in_dim(states, me_tp * share, share, 1)
    tokens = lax.all_gather(tokens, Z, axis=0, tiled=True)
    other_tokens = lax.ppermute(tokens, "tp", [(0, 1), (1, 0)])

    gradient = grad.astype(jnp.float32)
    squares = gradient * gradient + 1e-30
    row_partial = jnp.sum(squares, axis=1)
    col_partial = jnp.sum(squares, axis=0).reshape(-1, LANES)
    row_total = row_partial + lax.ppermute(row_partial, "tp", [(0, 1), (1, 0)])
    new_rows = 0.8 * row_moment + 0.2 * (row_total / columns)
    quarter = scatter_sum(col_partial, X)
    n_quarter = quarter.shape[0]
    extra = jnp.concatenate([scale, jnp.zeros((LANES - 1 - scale.shape[0],), jnp.float32), jnp.sum(new_rows).reshape(1)])
    mine = jnp.concatenate([quarter, jnp.broadcast_to(extra, (8, LANES))])
    theirs = lax.all_to_all(jnp.broadcast_to(mine, (n_z, *mine.shape)), Z, 0, 0)
    scales = theirs[:, n_quarter, : scale.shape[0]].reshape(-1, 1)
    mine = theirs.sum(axis=0)
    pieces = [shifted(mine, X, k) for k in steps(n_x)]
    new_weight, new_columns, *sends = apply_update(
        pieces, me_x, col_moment.reshape(-1, LANES), new_rows, grad, weight, n_z, rows
    )

    normed = jnp.zeros((n_x, tokens.shape[0], piece), jnp.bfloat16)
    for part, half in ((tokens, me_tp), (other_tokens, n_tp - 1 - me_tp)):
        gain = lax.dynamic_slice_in_dim(norm_gain, half * share, share, 0).astype(jnp.float32)
        part = (part.astype(jnp.float32) * scales * gain).astype(jnp.bfloat16)
        for i in range(share // piece):
            block = part[:, i * piece : (i + 1) * piece]
            normed = lax.dynamic_update_index_in_dim(normed, block, half * (share // piece) + i, 0)
    normed = lax.optimization_barrier(normed)

    ups = []
    for send in sends:
        block = lax.all_to_all(send, Z, 0, 0).reshape(-1, send.shape[2])
        if ups:
            block, ups[-1] = lax.optimization_barrier((block, ups[-1]))
        up = 0
        for k in steps(n_x):
            moved = shifted(block, X, k)
            source = lax.rem(me_x - k + n_x, n_x)
            up += dot(lax.dynamic_index_in_dim(normed, source, 0, keepdims=False), moved)
        ups.append(up.astype(jnp.bfloat16))
    hidden = None
    for c, up in enumerate(ups):
        up = lax.all_to_all(up.reshape(n_z, -1, up.shape[1]), Z, 0, 0)
        hidden = finish(up, gate_values, hidden, c)
    return (new_weight, new_rows, new_columns.reshape(-1), hidden)


def solution(mesh):
    job, fsdp, tp = (mesh.shape[n] for n in ("job", "fsdp", "tp"))
    finer = Mesh(mesh.devices.reshape(job, 4, fsdp // 4, tp), ("job", X, Z, "tp"))
    placed = (
        P(JOB_FSDP, "tp"),
        P(JOB_FSDP, "tp"),
        P(JOB_FSDP),
        P(("job", "tp")),
        P(JOB_FSDP, None),
        P("job"),
        P(JOB_FSDP, "tp"),
    )
    return jax.shard_map(
        step,
        mesh=finer,
        in_specs=placed,
        out_specs=(P(JOB_FSDP, "tp"), P(JOB_FSDP), P(("job", "tp")), P(JOB_FSDP, "tp")),
        check_vma=False,
    )
```

```python
import jax
import jax.numpy as jnp
from jax import lax
from jax.experimental import pallas as pl
from jax.experimental.pallas import tpu as pltpu
from jax.sharding import Mesh
from jax.sharding import PartitionSpec as P

JOB_FSDP = ("job", "fsdp_0", "fsdp_1")
X, Z = "fsdp_0", "fsdp_1"
CHUNKS = 2
LANES = 128
VMEM_LIMIT = 16 * 2**20
UPDATE_VMEM_LIMIT = 60500 * 2**10


def steps(size):
    return sorted(range(size), key=lambda k: min(k, size - k))


def shifted(x, axis, step):
    size = lax.axis_size(axis)
    return x if step == 0 else lax.ppermute(x, axis, [(i, (i + step) % size) for i in range(size)])


def scatter_sum(x, axis):
    size, me = lax.axis_size(axis), lax.axis_index(axis)
    blocks = x.reshape(size, -1, x.shape[1])
    total = 0
    for step in steps(size):
        block = lax.dynamic_index_in_dim(blocks, lax.rem(me + step, size), 0, keepdims=False)
        total += shifted(block, axis, step)
    return total


def vmem(n):
    return [pl.BlockSpec(memory_space=pltpu.VMEM)] * n


def apply_update(pieces, me, col_moment, new_rows, grad, weight, n_z, rows):
    size, local_rows, local_columns = len(pieces), *grad.shape
    share = col_moment.shape[0] // size
    width = local_columns // CHUNKS // n_z

    half = local_columns // 2

    def kernel(me_ref, *refs):
        piece_refs, refs = refs[:size], refs[size:]
        rows_ref, moment_hbm, grad_hbm, weight_hbm, out_ref, columns_ref, *send_refs = refs[: 6 + CHUNKS]
        factor_ref, moment_ref, grad_ref, weight_ref, moment_sem, sems = refs[6 + CHUNKS :]
        moment_copy = pltpu.make_async_copy(moment_hbm, moment_ref, moment_sem)
        moment_copy.start()
        copies = []
        for i in range(2):
            part = pl.ds(i * half, half)
            for j, (source, target) in enumerate(((grad_hbm, grad_ref), (weight_hbm, weight_ref))):
                copies.append(pltpu.make_async_copy(source.at[:, part], target.at[:, part], sems.at[i, j]))
                copies[-1].start()
        rows_summed = 0.0
        for step, piece_ref in zip(steps(size), piece_refs, strict=True):
            source = lax.rem(me_ref[0] - step + size, size)
            place = pl.ds(pl.multiple_of(source * share, share), share)
            factor_ref[place, :] = piece_ref[:share, :]
            rows_summed += piece_ref[share : share + 1, LANES - 1 :]
        moment_copy.wait()
        new_columns = 0.8 * moment_ref[...] + 0.2 * (factor_ref[...] / rows)
        columns_ref[...] = new_columns
        factor_ref[...] = 0.01 * jnp.sqrt((rows_summed / rows) / new_columns)
        row_factor = jnp.broadcast_to(1.0 / jnp.sqrt(rows_ref[...]), (local_rows, LANES))
        for group in range(local_columns // LANES):
            at = group * LANES
            if at % half == 0:
                for copy in copies[2 * (at // half) : 2 * (at // half) + 2]:
                    copy.wait()
            part = slice(at, at + LANES)
            scaled = grad_ref[:, part].astype(jnp.float32) * row_factor * factor_ref[group : group + 1, :]
            new = (weight_ref[:, part].astype(jnp.float32) - scaled).astype(jnp.bfloat16)
            out_ref[:, part] = new
            chunk, rest = divmod(at, width * n_z)
            target, rest = divmod(rest, width)
            send_refs[chunk][target, :, rest : rest + LANES] = new

    send = jax.ShapeDtypeStruct((n_z, local_rows, width), jnp.bfloat16)
    return pl.pallas_call(
        kernel,
        out_shape=[
            jax.ShapeDtypeStruct(grad.shape, jnp.bfloat16),
            jax.ShapeDtypeStruct(col_moment.shape, jnp.float32),
            *[send] * CHUNKS,
        ],
        in_specs=[
            pl.BlockSpec(memory_space=pltpu.SMEM),
            *vmem(size + 1),
            *[pl.BlockSpec(memory_space=pltpu.HBM)] * 3,
        ],
        out_specs=vmem(2 + CHUNKS),
        scratch_shapes=[
            pltpu.VMEM(col_moment.shape, jnp.float32),
            pltpu.VMEM(col_moment.shape, jnp.float32),
            pltpu.VMEM(grad.shape, grad.dtype),
            pltpu.VMEM(weight.shape, weight.dtype),
            pltpu.SemaphoreType.DMA,
            pltpu.SemaphoreType.DMA((2, 2)),
        ],
        cost_estimate=pl.CostEstimate(flops=6 * grad.size, bytes_accessed=8 * grad.size, transcendentals=0),
        compiler_params=pltpu.CompilerParams(vmem_limit_bytes=UPDATE_VMEM_LIMIT),
    )(me.reshape(1), *pieces, new_rows.reshape(-1, 1), col_moment, grad, weight)


def gather(x, axis):
    size, me = lax.axis_size(axis), lax.axis_index(axis)
    out = jnp.zeros((size, *x.shape), x.dtype)
    for k in steps(size):
        out = lax.dynamic_update_index_in_dim(out, shifted(x, axis, k), lax.rem(me - k + size, size), 0)
    return out


def dot(a, b):
    return jnp.dot(a, b, preferred_element_type=jnp.float32)


def finish(up, gate, hidden, chunk):
    n_z, tokens, width = up.shape

    def kernel(up_ref, gate_ref, *refs):
        out_ref = refs[-1]
        for z in range(n_z):
            part = slice(z * width, (z + 1) * width)
            v = gate_ref[:, part].astype(jnp.float32)
            out_ref[:, part] = (v / (1.0 + jnp.exp(-v)) * up_ref[z].astype(jnp.float32)).astype(jnp.bfloat16)

    block = pl.BlockSpec((tokens, n_z * width), lambda i: (0, chunk))
    first = hidden is None
    return pl.pallas_call(
        kernel,
        grid=(1,),
        out_shape=jax.ShapeDtypeStruct(gate.shape, jnp.bfloat16),
        in_specs=[pl.BlockSpec(up.shape, lambda i: (0, 0, 0)), block]
        + ([] if first else [pl.BlockSpec(memory_space=pl.ANY)]),
        out_specs=block,
        input_output_aliases={} if first else {2: 0},
        compiler_params=pltpu.CompilerParams(vmem_limit_bytes=VMEM_LIMIT),
    )(up, gate, *([] if first else [hidden]))


def step(weight, grad, row_moment, col_moment, states, norm_gain, gate_values):
    n_x, n_z, n_tp = lax.axis_size(X), lax.axis_size(Z), lax.axis_size("tp")
    me_x, me_tp = lax.axis_index(X), lax.axis_index("tp")
    local_rows, local_columns = grad.shape
    columns = local_columns * n_tp
    rows = local_rows * n_x * n_z
    gradient = grad.astype(jnp.float32)
    squares = gradient * gradient + 1e-30
    row_partial = jnp.sum(squares, axis=1)
    col_partial = jnp.sum(squares, axis=0).reshape(-1, LANES)
    features = states.shape[1]
    share = features // n_tp
    tokens = lax.dynamic_slice_in_dim(states, me_tp * share, share, 1)
    tokens = lax.all_gather(tokens, Z, axis=0, tiled=True)
    other_tokens = lax.ppermute(tokens, "tp", [(0, 1), (1, 0)])
    features = states.shape[1]
    share = features // n_tp
    tokens = lax.dynamic_slice_in_dim(states, me_tp * share, share, 1)
    tokens = lax.all_gather(tokens, Z, axis=0, tiled=True)
    other_tokens = lax.ppermute(tokens, "tp", [(0, 1), (1, 0)])
    values = states.astype(jnp.float32)
    scale = lax.rsqrt(jnp.mean(values * values, axis=1) + 1e-06)
    row_total = row_partial + lax.ppermute(row_partial, "tp", [(0, 1), (1, 0)])
    new_rows = 0.8 * row_moment + 0.2 * (row_total / columns)
    quarter = scatter_sum(col_partial, X)
    n_quarter = quarter.size
    tail = jnp.zeros((LANES,), jnp.float32).at[-1].set(jnp.sum(new_rows))
    mine = jnp.concatenate([quarter.reshape(-1), tail])
    theirs = lax.all_to_all(jnp.broadcast_to(mine, (n_z, *mine.shape)), Z, 0, 0)
    mine = theirs.sum(axis=0)
    tail = jnp.broadcast_to(mine[n_quarter:], (8, LANES))
    mine = jnp.concatenate([mine[:n_quarter].reshape(-1, LANES), tail])
    pieces = [shifted(mine, X, k) for k in steps(n_x)]
    new_weight, new_columns, *sends = apply_update(
        pieces, me_x, col_moment.reshape(-1, LANES), new_rows, grad, weight, n_z, rows
    )

    mean = sum(jnp.sum(jnp.square(t.astype(jnp.float32)), axis=1, keepdims=True) for t in (tokens, other_tokens)) / features
    scales = lax.rsqrt(mean + 1e-06)
    normed = []
    for part, half in ((tokens, me_tp), (other_tokens, n_tp - 1 - me_tp)):
        gain = lax.dynamic_slice_in_dim(norm_gain, half * share, share, 0).astype(jnp.float32)
        normed.append((part.astype(jnp.float32) * scales * gain).astype(jnp.bfloat16))
    normed = lax.optimization_barrier(normed)

    ups = []
    for send in sends:
        block = lax.all_to_all(send, Z, 0, 0).reshape(-1, send.shape[2])
        if ups:
            block, ups[-1] = lax.optimization_barrier((block, ups[-1]))
        block = gather(block, X).reshape(rows, -1)
        up = dot(normed[0], lax.dynamic_slice_in_dim(block, me_tp * share, share, 0))
        up += dot(normed[1], lax.dynamic_slice_in_dim(block, (n_tp - 1 - me_tp) * share, share, 0))
        ups.append(up.astype(jnp.bfloat16).reshape(n_z, -1, up.shape[1]))
    hidden = None
    for c, up in enumerate(ups):
        up = lax.all_to_all(up, Z, 0, 0)
        hidden = finish(up, gate_values, hidden, c)
    return (new_weight, new_rows, new_columns.reshape(-1), hidden)


def solution(mesh):
    job, fsdp, tp = (mesh.shape[n] for n in ("job", "fsdp", "tp"))
    finer = Mesh(mesh.devices.reshape(job, 4, fsdp // 4, tp), ("job", X, Z, "tp"))
    placed = (
        P(JOB_FSDP, "tp"),
        P(JOB_FSDP, "tp"),
        P(JOB_FSDP),
        P(("job", "tp")),
        P(JOB_FSDP, None),
        P("job"),
        P(JOB_FSDP, "tp"),
    )
    return jax.shard_map(
        step,
        mesh=finer,
        in_specs=placed,
        out_specs=(P(JOB_FSDP, "tp"), P(JOB_FSDP), P(("job", "tp")), P(JOB_FSDP, "tp")),
        check_vma=False,
    )
```

```python
import jax
import jax.numpy as jnp
from jax import lax
from jax.experimental import pallas as pl
from jax.experimental.pallas import tpu as pltpu
from jax.sharding import Mesh
from jax.sharding import PartitionSpec as P

JOB_FSDP = ("job", "fsdp_0", "fsdp_1")
X, Z = "fsdp_0", "fsdp_1"
CHUNKS = 2
LANES = 128
VMEM_LIMIT = 16 * 2**20
UPDATE_VMEM_LIMIT = 60500 * 2**10


def steps(size):
    return sorted(range(size), key=lambda k: min(k, size - k))


def shifted(x, axis, step):
    size = lax.axis_size(axis)
    return x if step == 0 else lax.ppermute(x, axis, [(i, (i + step) % size) for i in range(size)])


def scatter_sum(x, axis):
    size, me = lax.axis_size(axis), lax.axis_index(axis)
    blocks = x.reshape(size, -1, x.shape[1])
    total = 0
    for step in steps(size):
        block = lax.dynamic_index_in_dim(blocks, lax.rem(me + step, size), 0, keepdims=False)
        total += shifted(block, axis, step)
    return total


def vmem(n):
    return [pl.BlockSpec(memory_space=pltpu.VMEM)] * n


def apply_update(pieces, me, col_moment, new_rows, grad, weight, n_z, rows):
    size, local_rows, local_columns = len(pieces), *grad.shape
    share = col_moment.shape[0] // size
    width = local_columns // CHUNKS // n_z

    half = local_columns // 2

    def kernel(me_ref, *refs):
        piece_refs, refs = refs[:size], refs[size:]
        rows_ref, moment_hbm, grad_hbm, weight_hbm, out_ref, columns_ref, *send_refs = refs[: 6 + CHUNKS]
        factor_ref, moment_ref, grad_ref, weight_ref, moment_sem, sems = refs[6 + CHUNKS :]
        moment_copy = pltpu.make_async_copy(moment_hbm, moment_ref, moment_sem)
        moment_copy.start()
        copies = []
        for i in range(2):
            part = pl.ds(i * half, half)
            for j, (source, target) in enumerate(((grad_hbm, grad_ref), (weight_hbm, weight_ref))):
                copies.append(pltpu.make_async_copy(source.at[:, part], target.at[:, part], sems.at[i, j]))
                copies[-1].start()
        rows_summed = 0.0
        for step, piece_ref in zip(steps(size), piece_refs, strict=True):
            source = lax.rem(me_ref[0] - step + size, size)
            place = pl.ds(pl.multiple_of(source * share, share), share)
            factor_ref[place, :] = piece_ref[:share, :]
            rows_summed += piece_ref[share : share + 1, LANES - 1 :]
        moment_copy.wait()
        new_columns = 0.8 * moment_ref[...] + 0.2 * (factor_ref[...] / rows)
        columns_ref[...] = new_columns
        factor_ref[...] = 0.01 * jnp.sqrt((rows_summed / rows) / new_columns)
        row_factor = jnp.broadcast_to(1.0 / jnp.sqrt(rows_ref[...]), (local_rows, LANES))
        for group in range(local_columns // LANES):
            at = group * LANES
            if at % half == 0:
                for copy in copies[2 * (at // half) : 2 * (at // half) + 2]:
                    copy.wait()
            part = slice(at, at + LANES)
            scaled = grad_ref[:, part].astype(jnp.float32) * row_factor * factor_ref[group : group + 1, :]
            new = (weight_ref[:, part].astype(jnp.float32) - scaled).astype(jnp.bfloat16)
            out_ref[:, part] = new
            chunk, rest = divmod(at, width * n_z)
            target, rest = divmod(rest, width)
            send_refs[chunk][target, :, rest : rest + LANES] = new

    send = jax.ShapeDtypeStruct((n_z, local_rows, width), jnp.bfloat16)
    return pl.pallas_call(
        kernel,
        out_shape=[
            jax.ShapeDtypeStruct(grad.shape, jnp.bfloat16),
            jax.ShapeDtypeStruct(col_moment.shape, jnp.float32),
            *[send] * CHUNKS,
        ],
        in_specs=[
            pl.BlockSpec(memory_space=pltpu.SMEM),
            *vmem(size + 1),
            *[pl.BlockSpec(memory_space=pltpu.HBM)] * 3,
        ],
        out_specs=vmem(2 + CHUNKS),
        scratch_shapes=[
            pltpu.VMEM(col_moment.shape, jnp.float32),
            pltpu.VMEM(col_moment.shape, jnp.float32),
            pltpu.VMEM(grad.shape, grad.dtype),
            pltpu.VMEM(weight.shape, weight.dtype),
            pltpu.SemaphoreType.DMA,
            pltpu.SemaphoreType.DMA((2, 2)),
        ],
        cost_estimate=pl.CostEstimate(flops=6 * grad.size, bytes_accessed=8 * grad.size, transcendentals=0),
        compiler_params=pltpu.CompilerParams(vmem_limit_bytes=UPDATE_VMEM_LIMIT),
    )(me.reshape(1), *pieces, new_rows.reshape(-1, 1), col_moment, grad, weight)


def gather(x, axis):
    size, me = lax.axis_size(axis), lax.axis_index(axis)
    out = jnp.zeros((size, *x.shape), x.dtype)
    for k in steps(size):
        moved = shifted(x, axis, k)
        out = lax.dynamic_update_index_in_dim(out, moved, lax.rem(me - k + size, size), 0)
    return out


def dot(a, b):
    return jnp.dot(a, b, preferred_element_type=jnp.float32)


def finish(up, gate, hidden, chunk):
    n_z, tokens, width = up.shape

    def kernel(up_ref, gate_ref, *refs):
        out_ref = refs[-1]
        for z in range(n_z):
            part = slice(z * width, (z + 1) * width)
            v = gate_ref[:, part].astype(jnp.float32)
            out_ref[:, part] = (v / (1.0 + jnp.exp(-v)) * up_ref[z].astype(jnp.float32)).astype(jnp.bfloat16)

    block = pl.BlockSpec((tokens, n_z * width), lambda i: (0, chunk))
    first = hidden is None
    return pl.pallas_call(
        kernel,
        grid=(1,),
        out_shape=jax.ShapeDtypeStruct(gate.shape, jnp.bfloat16),
        in_specs=[pl.BlockSpec(up.shape, lambda i: (0, 0, 0)), block]
        + ([] if first else [pl.BlockSpec(memory_space=pl.ANY)]),
        out_specs=block,
        input_output_aliases={} if first else {2: 0},
        compiler_params=pltpu.CompilerParams(vmem_limit_bytes=VMEM_LIMIT),
    )(up, gate, *([] if first else [hidden]))


def step(weight, grad, row_moment, col_moment, states, norm_gain, gate_values):
    n_x, n_z, n_tp = lax.axis_size(X), lax.axis_size(Z), lax.axis_size("tp")
    me_x, me_tp = lax.axis_index(X), lax.axis_index("tp")
    local_rows, local_columns = grad.shape
    columns = local_columns * n_tp
    rows = local_rows * n_x * n_z
    gradient = grad.astype(jnp.float32)
    squares = gradient * gradient + 1e-30
    row_partial = jnp.sum(squares, axis=1)
    col_partial = jnp.sum(squares, axis=0).reshape(-1, LANES)
    features = states.shape[1]
    share = features // n_tp
    tokens = lax.dynamic_slice_in_dim(states, me_tp * share, share, 1)
    tokens = lax.all_gather(tokens, Z, axis=0, tiled=True)
    other_tokens = lax.ppermute(tokens, "tp", [(0, 1), (1, 0)])
    features = states.shape[1]
    share = features // n_tp
    tokens = lax.dynamic_slice_in_dim(states, me_tp * share, share, 1)
    tokens = lax.all_gather(tokens, Z, axis=0, tiled=True)
    other_tokens = lax.ppermute(tokens, "tp", [(0, 1), (1, 0)])
    values = states.astype(jnp.float32)
    scale = lax.rsqrt(jnp.mean(values * values, axis=1) + 1e-06)
    row_total = row_partial + lax.ppermute(row_partial, "tp", [(0, 1), (1, 0)])
    new_rows = 0.8 * row_moment + 0.2 * (row_total / columns)
    quarter = scatter_sum(col_partial, X)
    n_quarter = quarter.size
    values = states.astype(jnp.float32)
    scale = lax.rsqrt(jnp.mean(values * values, axis=1) + 1e-06)
    gap = jnp.zeros((LANES - 1 - scale.size,), jnp.float32)
    tail = jnp.concatenate([scale, gap, jnp.sum(new_rows).reshape(1)])
    mine = jnp.concatenate([quarter.reshape(-1), tail])
    theirs = lax.all_to_all(jnp.broadcast_to(mine, (n_z, *mine.shape)), Z, 0, 0)
    scales = theirs[:, n_quarter : n_quarter + scale.size].reshape(-1, 1)
    mine = theirs.sum(axis=0)
    tail = jnp.broadcast_to(mine[n_quarter:], (8, LANES))
    mine = jnp.concatenate([mine[:n_quarter].reshape(-1, LANES), tail])
    pieces = [shifted(mine, X, k) for k in steps(n_x)]
    new_weight, new_columns, *sends = apply_update(
        pieces, me_x, col_moment.reshape(-1, LANES), new_rows, grad, weight, n_z, rows
    )

    normed = []
    for part, half in ((tokens, me_tp), (other_tokens, n_tp - 1 - me_tp)):
        gain = lax.dynamic_slice_in_dim(norm_gain, half * share, share, 0).astype(jnp.float32)
        normed.append((part.astype(jnp.float32) * scales * gain).astype(jnp.bfloat16))
    normed = lax.optimization_barrier(normed)

    ups = []
    for send in sends:
        block = lax.all_to_all(send, Z, 0, 0).reshape(-1, send.shape[2])
        if ups:
            block, ups[-1] = lax.optimization_barrier((block, ups[-1]))
        block = gather(block, X).reshape(rows, -1)
        up = dot(normed[0], lax.dynamic_slice_in_dim(block, me_tp * share, share, 0))
        up += dot(normed[1], lax.dynamic_slice_in_dim(block, (n_tp - 1 - me_tp) * share, share, 0))
        ups.append(up.astype(jnp.bfloat16).reshape(n_z, -1, up.shape[1]))
    hidden = None
    for c, up in enumerate(ups):
        up = lax.all_to_all(up, Z, 0, 0)
        hidden = finish(up, gate_values, hidden, c)
    return (new_weight, new_rows, new_columns.reshape(-1), hidden)


def solution(mesh):
    job, fsdp, tp = (mesh.shape[n] for n in ("job", "fsdp", "tp"))
    finer = Mesh(mesh.devices.reshape(job, 4, fsdp // 4, tp), ("job", X, Z, "tp"))
    placed = (
        P(JOB_FSDP, "tp"),
        P(JOB_FSDP, "tp"),
        P(JOB_FSDP),
        P(("job", "tp")),
        P(JOB_FSDP, None),
        P("job"),
        P(JOB_FSDP, "tp"),
    )
    return jax.shard_map(
        step,
        mesh=finer,
        in_specs=placed,
        out_specs=(P(JOB_FSDP, "tp"), P(JOB_FSDP), P(("job", "tp")), P(JOB_FSDP, "tp")),
        check_vma=False,
    )
```
